256 devices in a mesh: row: 8 (over z), col: 32 (over y, x, core).
Axes of the slice: x: 4, y: 4, z: 8, core: 2. Of those that a mesh axis runs over, the one named last changes fastest.
Arguments:
- factor: bfloat16 [131072, 5, 1024], P('col', None, 'row'), may hold values from -0.0625 to 0.0625
- diag_inverse: bfloat16 [5, 1024, 1024], P(None, 'row'), may hold values from -1 to 2
- right_side: float32 [16, 128, 1024], P(None, 'col', 'row'), may hold values from -6 to 6
- tile_order: int32 [128], replicated, may hold values from 0 to 127, each once
- live_segments: int32 [16], replicated, may hold values from 2 to 5
Outputs:
- result: float32 [16, 128, 1024], P(None, 'col', 'row')
The draws below stay inside these ranges and needn't reach their ends.
Inputs may be any that keep to these rules, and one draw needn't show every extreme that they name: `tile_order`: each of 0 to 127 appears once.
All inputs are finite; a program needn't handle non-finite values.
Results may differ from the reference program's by a relative error of at most 0.0019.
Values may be sent and summed in bfloat16 or wider, within the bound.
A program may use at most 64 MiB of HBM per device.

```python
import math
import jax
import jax.numpy as jnp
from jax import lax

TB = 1024
NRHS = 16
SECTIONS = 5
K = 128
N = 131072


def draw_diag_inverse(key, part):
    identity = jnp.broadcast_to(jnp.eye(TB, dtype=jnp.float32), (SECTIONS, TB, TB))
    noise = jax.random.normal(key, (SECTIONS, TB, TB), jnp.float32) * (0.4 / math.sqrt(TB))
    return (identity + noise).astype(jnp.bfloat16)


def place_ends(values, stream_key, low, top_value):
    shape = values.shape
    place = [jax.random.randint(jax.random.fold_in(stream_key, axis), (), 0, shape[axis]) for axis in range(len(shape))]
    values = values.at[tuple(place)].set(low)
    longest = shape.index(max(shape))
    place[longest] = (place[longest] + 1) % shape[longest]
    return values.at[tuple(place)].set(top_value)


def level_of(own_key, shape, cuts, least, high):
    gain = 1.0
    for position, blocks in cuts:
        heights = jax.random.uniform(jax.random.fold_in(jax.random.fold_in(own_key, 6), position), (blocks,), jnp.float32, least / len(cuts), high / len(cuts))
        gain = gain * jnp.repeat(jnp.exp(heights), shape[position] // blocks).reshape((-1,) + (1,) * (len(shape) - 1 - position))
    return gain


def scatter_about(rng, extent, scale, limit, cuts=(), kind=jnp.bfloat16):
    loudness = level_of(rng, extent, cuts, -0.22, 0.18) if cuts else 1.0
    entries = jax.random.normal(rng, extent, jnp.float32) * scale * loudness
    return jnp.minimum(jnp.maximum(entries, -limit), limit).astype(kind)


def setup_inputs(seed: int = 0) -> dict:
    key_of = jax.random.split(jax.random.key(seed), 6)
    factor = scatter_about(key_of[0], (N, SECTIONS, TB), (2 * SECTIONS * TB) ** -0.5, 0.0625, ((0, 32), (2, 8)))
    diag_inverse = draw_diag_inverse(jax.random.fold_in(key_of[5], 71), 0)
    right_side = scatter_about(key_of[2], (NRHS, K, TB), 1.0, 6.0, ((1, 32), (2, 8)), jnp.float32)
    tile_order = jax.random.permutation(key_of[3], K).astype(jnp.int32)
    live_segments = place_ends(jax.random.randint(key_of[4], (NRHS,), SECTIONS // 2, SECTIONS + 1), jax.random.fold_in(key_of[4], 1), SECTIONS // 2, SECTIONS).astype(jnp.int32)
    return dict(factor=factor, diag_inverse=diag_inverse, right_side=right_side, tile_order=tile_order, live_segments=live_segments)


def reference(factor, diag_inverse, right_side, tile_order, live_segments):
    segment_limit = live_segments.astype(jnp.int32)
    partial_value = jnp.zeros((NRHS, K * TB), jnp.float32)
    result = jnp.zeros((NRHS, K, TB), jnp.float32)
    for section in range(SECTIONS):
        slot_id = tile_order[section].astype(jnp.int32)
        offset = (slot_id * TB).astype(jnp.int32)
        rhs_tile = lax.dynamic_index_in_dim(right_side, slot_id, 1, keepdims=False)
        remaining = rhs_tile - lax.dynamic_slice_in_dim(partial_value, offset, TB, 1)
        inverse = diag_inverse[section].astype(jnp.float32)
        solved = lax.dot_general(remaining, inverse, (((1,), (1,)), ((), ())),
                                 precision=lax.Precision.HIGHEST, preferred_element_type=jnp.float32)
        is_live = (section < segment_limit)[:, None]
        sent_block = jnp.where(is_live, solved, jnp.zeros_like(solved)).astype(jnp.bfloat16)
        partial_value = partial_value + lax.dot_general(sent_block, factor[:, section, :], (((1,), (1,)), ((), ())),
                                            preferred_element_type=jnp.float32)
        stored = jnp.where(is_live, solved, remaining)
        result = lax.dynamic_update_slice_in_dim(result, stored[:, None, :], slot_id, 1)
    slot_ids = jnp.arange(K, dtype=jnp.int32)
    visited = jnp.any(slot_ids[:, None] == tile_order[:SECTIONS][None, :], axis=1)
    trailing = right_side - partial_value.reshape(NRHS, K, TB)
    return jnp.where(visited[None, :, None], result, trailing)
```

```python
import functools
import jax
import jax.numpy as jnp
from jax import lax
from jax.experimental import pallas as pl
from jax.experimental.pallas import tpu as pltpu
from jax.sharding import PartitionSpec as P

MESH = pl.DeviceIdType.MESH
SPARE = 128
DEPTH = 3
NT = (((1,), (1,)), ((), ()))


def encode(value, spare):
    peak = jnp.max(jnp.abs(value), axis=1, keepdims=True)
    power = jnp.ceil(jnp.log2(jnp.maximum(peak, 1e-30)))
    coded = jnp.floor(value * jnp.exp2(14.0 - power) + 0.5)
    powers = jnp.broadcast_to(power, (value.shape[0], spare))
    both = jnp.concatenate([coded, powers], axis=1)
    return both.astype(jnp.int32).astype(jnp.int16)


def decode(coded, count):
    numbers = coded.astype(jnp.int32).astype(jnp.float32)
    scale = jnp.exp2(numbers[:, count:count + 1] - 14.0)
    return numbers[:, :count] * scale


def ring_order(count):
    return sorted(range(1, count), key=lambda d: -min(d, count - d))


def remote(src, dst, send_sem, recv_sem, device):
    return pltpu.make_async_remote_copy(
        src_ref=src, dst_ref=dst, send_sem=send_sem, recv_sem=recv_sem,
        device_id=device, device_id_type=MESH,
    )


def dot_nt(a, b):
    return lax.dot_general(a, b, NT, preferred_element_type=jnp.float32)


def kernel(
    rows, cols, blocks, factor_hbm, inverse_hbm, rhs_hbm, order_hbm, live_hbm, out,
    factor, inverse, cand, theirs, pieces, mine, panels,
    b_own, b_pair, b_chip, b0_in, b1_in, b0_all, b1_all,
    part_out, part_in, stored, acc, tail_out, tail_in, rhs, order, live,
    factor_sem, inverse_sem, small_sem, pair_sems, b_sems, piece_sems, panel_sems,
    b0_sems, b1_sems, part_sems, stored_sems, tail_sems,
):
    sections = len(factor)
    rows_dev, tile, width = factor[0].shape
    rhs_count = rhs.shape[0]
    chips = cols // 2
    piece = tile // chips
    r, c = lax.axis_index("row"), lax.axis_index("col")
    chip, core = lax.div(c, 2), lax.rem(c, 2)
    index = {tu: i for i, tu in enumerate(blocks)}

    small = (
        pltpu.make_async_copy(rhs_hbm, rhs, small_sem.at[0]),
        pltpu.make_async_copy(order_hbm, order, small_sem.at[1]),
        pltpu.make_async_copy(live_hbm, live, small_sem.at[2]),
    )
    for copy in small:
        copy.start()
    factor_loads = []
    for u in range(sections):
        copy = pltpu.make_async_copy(factor_hbm.at[u], factor[u], factor_sem.at[u])
        copy.start()
        factor_loads.append(copy)
    inverse_load = pltpu.make_async_copy(inverse_hbm, inverse, inverse_sem.at[0])
    inverse_load.start()

    barrier = pltpu.get_barrier_semaphore()
    for axis, me, count in (("row", r, rows), ("col", c, cols)):
        for d in range(1, count):
            pl.semaphore_signal(
                barrier, inc=1, device_id={axis: lax.rem(me + d, count)}, device_id_type=MESH
            )

    for copy in small:
        copy.wait()
    slots = [order[u] for u in range(sections)]
    locals_ = [lax.rem(s, rows_dev) for s in slots]
    root_core = [lax.rem(lax.div(s, rows_dev), 2) for s in slots]
    root_chip = [lax.div(s, 2 * rows_dev) for s in slots]
    row_ids = lax.broadcasted_iota(jnp.int32, (rhs_count, width), 0)
    limit = jnp.zeros((rhs_count, width), jnp.int32)
    for k in range(rhs_count):
        limit = jnp.where(row_ids == k, live[k], limit)

    for t in range(sections):
        picked = rhs[:, 0, :]
        for j in range(1, rows_dev):
            picked = jnp.where(locals_[t] == j, rhs[:, j, :], picked)
        b_own[t] = picked
    for copy in factor_loads + [inverse_load]:
        copy.wait()

    peers = [lax.rem(r + d, rows) for d in ring_order(rows)]
    others = [lax.rem(chip + d, chips) for d in range(1, chips)]

    def trail(t, sent):
        for j in range(rows_dev):
            update = dot_nt(sent, factor[t][j])
            if t == 0:
                acc[j] = update
            else:
                acc[j] += update

    @pl.when(core == 0)
    def _():
        pl.semaphore_wait(barrier, rows - 1 + cols - 1)
        pair = remote(b_own, b_pair, b_sems.at[0], b_sems.at[1], {"col": c + 1})
        pair.start()

        def scatter(i):
            t, u = blocks[i]
            remote(
                theirs[i], theirs[i], pair_sems.at[0, i], pair_sems.at[1, i], {"col": c + 1}
            ).wait_recv()
            for s in range(0, tile, 256):
                own = factor[u][locals_[t], pl.ds(s, 256), :]
                cand[i][s:s + 256] = jnp.where(
                    root_core[t] == 1, theirs[i][s:s + 256], own
                )
            for p in others:
                remote(
                    cand[i].at[pl.ds(pl.multiple_of(p * piece, piece), piece)],
                    pieces[i].at[chip], piece_sems.at[0, i], piece_sems.at[1, i],
                    {"col": 2 * p},
                ).start()
            pieces[i][chip] = cand[i][pl.ds(pl.multiple_of(chip * piece, piece), piece)]

        def gather(i):
            t, u = blocks[i]
            some = pieces[i].at[pl.ds(0, chips - 1)]
            remote(some, some, piece_sems.at[0, i], piece_sems.at[1, i], {"col": c + 1}).wait_recv()
            mine[i] = pieces[i][root_chip[t]]
            here = pl.ds(pl.multiple_of(chip * piece, piece), piece)
            for p in [chip] + others:
                remote(
                    mine.at[i], panels[i].at[here], panel_sems.at[0, i], panel_sems.at[1, i],
                    {"col": 2 * p + 1},
                ).start()

        for i in range(min(DEPTH, len(blocks))):
            scatter(i)
        for i in range(len(blocks)):
            gather(i)
            if i + DEPTH < len(blocks):
                scatter(i + DEPTH)

        for t in range(sections):
            remote(
                stored.at[t], stored.at[t], stored_sems.at[0, t], stored_sems.at[1, t],
                {"col": c + 1},
            ).wait_recv()
            trail(t, jnp.where(limit > t, stored[t], 0.0).astype(jnp.bfloat16))

        pair.wait_send()
        for i in range(len(blocks)):
            some = pieces[i].at[pl.ds(0, chips - 1)]
            remote(some, some, piece_sems.at[0, i], piece_sems.at[1, i], {"col": c + 1}).wait_send()
            remote(
                panels[i], panels[i], panel_sems.at[0, i], panel_sems.at[1, i], {"col": c + 1}
            ).wait_send()

    @pl.when(core == 1)
    def _():
        for i, (t, u) in enumerate(blocks):
            for s in range(0, tile, 256):
                cand[i][s:s + 256] = factor[u][locals_[t], pl.ds(s, 256), :]
        pl.semaphore_wait(barrier, rows - 1 + cols - 1)
        remote(b_own, b_pair, b_sems.at[0], b_sems.at[1], {"col": c - 1}).wait_recv()
        for t in range(sections):
            b_chip[t] = jnp.where(root_core[t] == 1, b_own[t], b_pair[t])
        for p in others:
            remote(
                b_chip.at[0], b0_in.at[chip], b0_sems.at[0, 0], b0_sems.at[1, 0],
                {"col": 2 * p + 1},
            ).start()
        pairs = []
        for i in range(len(blocks)):
            copy = remote(
                cand[i], theirs[i], pair_sems.at[0, i], pair_sems.at[1, i], {"col": c - 1}
            )
            copy.start()
            pairs.append(copy)
        later = b_chip.at[pl.ds(1, sections - 1)]
        for p in others:
            remote(
                later, b1_in.at[chip], b1_sems.at[0, 0], b1_sems.at[1, 0], {"col": 2 * p + 1}
            ).start()
        b0_in[chip] = b_chip[0]
        b1_in[chip] = b_chip[1:]

        some = b0_in.at[pl.ds(0, chips - 1)]
        b0_wait = remote(some, some, b0_sems.at[0, 0], b0_sems.at[1, 0], {"col": c - 1})
        b0_wait.wait_recv()
        b0_all[r] = b0_in[root_chip[0]]
        for peer in peers:
            remote(
                b0_all.at[r], b0_all.at[r], b0_sems.at[0, 1], b0_sems.at[1, 1], {"row": peer}
            ).start()
        some = b1_in.at[pl.ds(0, chips - 1)]
        b1_wait = remote(some, some, b1_sems.at[0, 0], b1_sems.at[1, 0], {"col": c - 1})
        b1_wait.wait_recv()
        for t in range(1, sections):
            b1_all[r, t - 1] = b1_in[root_chip[t], t - 1]
        for peer in peers:
            remote(
                b1_all.at[r], b1_all.at[r], b1_sems.at[0, 1], b1_sems.at[1, 1], {"row": peer}
            ).start()
        some = b0_all.at[pl.ds(0, rows - 1)]
        b0_row = remote(some, some, b0_sems.at[0, 1], b0_sems.at[1, 1], {"col": c - 1})
        some = b1_all.at[pl.ds(0, rows - 1)]
        b1_row = remote(some, some, b1_sems.at[0, 1], b1_sems.at[1, 1], {"col": c - 1})

        def panel(t, u):
            i = index[t, u]
            remote(
                panels[i], panels[i], panel_sems.at[0, i], panel_sems.at[1, i], {"col": c - 1}
            ).wait_recv()
            return panels[i][...]

        sents, pending = [], []
        own, older = None, None
        for t in range(sections):
            if t == 0:
                b0_row.wait_recv()
                remaining = jnp.concatenate([b0_all[s] for s in range(rows)], axis=1)
            else:
                remaining = jnp.concatenate(
                    [b1_all[s, t - 1] for s in range(rows)], axis=1
                ) - own
                for peer in reversed(peers):
                    remote(
                        part_out.at[t], part_in.at[t, peer], part_sems.at[0, t, peer],
                        part_sems.at[1, t, peer], {"row": peer},
                    ).wait_recv()
                    remaining = remaining - decode(part_in[t, peer], tile)
            kept = remaining[:, :width]
            for s in range(1, rows):
                kept = jnp.where(r == s, remaining[:, s * width:(s + 1) * width], kept)
            high = remaining.astype(jnp.bfloat16)
            rest = remaining - high.astype(jnp.float32)
            middle = rest.astype(jnp.bfloat16)
            low = (rest - middle.astype(jnp.float32)).astype(jnp.bfloat16)
            parts = dot_nt(jnp.concatenate([high, middle, low], axis=0), inverse[t])
            solved = (
                parts[2 * rhs_count:] + parts[rhs_count:2 * rhs_count]
            ) + parts[:rhs_count]
            is_live = limit > t
            sent = jnp.where(is_live, solved, 0.0).astype(jnp.bfloat16)
            sents.append(sent)
            if t + 1 < sections:
                own = dot_nt(sent, panel(t + 1, t))
                if older is not None:
                    own = own + older
                part_out[t + 1] = encode(own, SPARE)
                for peer in peers:
                    copy = remote(
                        part_out.at[t + 1], part_in.at[t + 1, r], part_sems.at[0, t + 1, peer],
                        part_sems.at[1, t + 1, r], {"row": peer},
                    )
                    copy.start()
                    pending.append(copy)
            stored[t] = jnp.where(is_live, solved, kept)
            copy = remote(
                stored.at[t], stored.at[t], stored_sems.at[0, t], stored_sems.at[1, t],
                {"col": c - 1},
            )
            copy.start()
            pending.append(copy)
            trail(t, sent)
            if t == 0:
                b1_row.wait_recv()
            if t + 2 < sections:
                older = dot_nt(sents[0], panel(t + 2, 0))
                for u in range(1, t + 1):
                    older = older + dot_nt(sents[u], panel(t + 2, u))

        for wait in (b0_wait, b1_wait, b0_row, b1_row):
            wait.wait_send()
        for copy in pairs + pending:
            copy.wait_send()

    spans = []
    totals = [acc[j] for j in range(rows_dev)]
    for s in range(rows):
        spans.append([x[:, s * width:(s + 1) * width] for x in totals])
        tail_out[s] = encode(jnp.concatenate(spans[s], axis=1), SPARE)
    tails = []
    for peer in peers:
        copy = remote(
            tail_out.at[peer], tail_in.at[r], tail_sems.at[0, peer], tail_sems.at[1, r],
            {"row": peer},
        )
        copy.start()
        tails.append(copy)
    values = []
    for j in range(rows_dev):
        total = spans[0][j]
        for s in range(1, rows):
            total = jnp.where(r == s, spans[s][j], total)
        values.append(rhs[:, j, :] - total)
    for peer in reversed(peers):
        remote(
            tail_out.at[peer], tail_in.at[peer], tail_sems.at[0, peer], tail_sems.at[1, peer],
            {"row": peer},
        ).wait_recv()
        other = decode(tail_in[peer], rows_dev * width)
        for j in range(rows_dev):
            values[j] = values[j] - other[:, j * width:(j + 1) * width]
    for j in range(rows_dev):
        value = values[j]
        for t in range(sections):
            value = jnp.where(slots[t] == c * rows_dev + j, stored[t], value)
        out[:, j, :] = value
    for copy in tails:
        copy.wait_send()


def per_device(rows, cols, factor, diag_inverse, right_side, tile_order, live_segments):
    sections, width, tile = diag_inverse.shape
    rhs_count, rows_dev, _ = right_side.shape
    panel = jnp.transpose(factor, (1, 0, 2)).reshape(sections, rows_dev, tile, width)
    blocks = [(t, u) for t in range(1, sections) for u in range(t)]
    count, chips = len(blocks), cols // 2
    vmem = pl.BlockSpec(memory_space=pltpu.VMEM)
    hbm = pl.BlockSpec(memory_space=pl.ANY)
    f32, bf16, i16 = jnp.float32, jnp.bfloat16, jnp.int16
    dma = pltpu.SemaphoreType.DMA
    return pl.pallas_call(
        functools.partial(kernel, rows, cols, blocks),
        out_shape=jax.ShapeDtypeStruct(right_side.shape, f32),
        in_specs=[hbm] * 5,
        out_specs=vmem,
        scratch_shapes=[
            [pltpu.VMEM((rows_dev, tile, width), bf16)] * sections,
            pltpu.VMEM((sections, width, tile), bf16),
            [pltpu.VMEM((tile, width), bf16)] * count,
            [pltpu.VMEM((tile, width), bf16)] * count,
            [pltpu.VMEM((chips, tile // chips, width), bf16)] * count,
            pltpu.VMEM((count, tile // chips, width), bf16),
            [pltpu.VMEM((tile, width), bf16)] * count,
            pltpu.VMEM((sections, rhs_count, width), f32),
            pltpu.VMEM((sections, rhs_count, width), f32),
            pltpu.VMEM((sections, rhs_count, width), f32),
            pltpu.VMEM((chips, rhs_count, width), f32),
            pltpu.VMEM((chips, sections - 1, rhs_count, width), f32),
            pltpu.VMEM((rows, rhs_count, width), f32),
            pltpu.VMEM((rows, sections - 1, rhs_count, width), f32),
            pltpu.VMEM((sections, rhs_count, tile + SPARE), i16),
            pltpu.VMEM((sections, rows, rhs_count, tile + SPARE), i16),
            pltpu.VMEM((sections, rhs_count, width), f32),
            pltpu.VMEM((rows_dev, rhs_count, tile), f32),
            pltpu.VMEM((rows, rhs_count, rows_dev * width + SPARE), i16),
            pltpu.VMEM((rows, rhs_count, rows_dev * width + SPARE), i16),
            pltpu.VMEM(right_side.shape, f32),
            pltpu.SMEM(tile_order.shape, jnp.int32),
            pltpu.SMEM(live_segments.shape, jnp.int32),
            dma((sections,)),
            dma((1,)),
            dma((3,)),
            dma((2, count)),
            dma((2,)),
            dma((2, count)),
            dma((2, count)),
            dma((2, 2)),
            dma((2, 2)),
            dma((2, sections, rows)),
            dma((2, sections)),
            dma((2, rows)),
        ],
        compiler_params=pltpu.CompilerParams(
            collective_id=0, has_side_effects=True, vmem_limit_bytes=67043328
        ),
    )(panel, diag_inverse, right_side, tile_order, live_segments)


def solution(mesh):
    return jax.shard_map(
        functools.partial(per_device, mesh.shape["row"], mesh.shape["col"]),
        mesh=mesh,
        in_specs=(P("col", None, "row"), P(None, "row", None), P(None, "col", "row"), P(), P()),
        out_specs=P(None, "col", "row"),
        check_vma=False,
    )
```

```python
import functools
import jax
import jax.numpy as jnp
from jax import lax
from jax.experimental import pallas as pl
from jax.experimental.pallas import tpu as pltpu
from jax.sharding import PartitionSpec as P

MESH = pl.DeviceIdType.MESH
SPARE = 128
SIDE = 4
DIRECT = 10
ORDER = "s0 s1 s2 s3 g0 s4 g1 s5 g2 s6 g3 s7 g4 s8 g5 s9 g6 g7 g8 g9"
NT = (((1,), (1,)), ((), ()))


def encode(value, spare):
    peak = jnp.max(jnp.abs(value), axis=1, keepdims=True)
    power = jnp.ceil(jnp.log2(jnp.maximum(peak, 1e-30)))
    coded = jnp.floor(value * jnp.exp2(14.0 - power) + 0.5)
    powers = jnp.broadcast_to(power, (value.shape[0], spare))
    both = jnp.concatenate([coded, powers], axis=1)
    return both.astype(jnp.int32).astype(jnp.int16)


def decode(coded, count):
    numbers = coded.astype(jnp.int32).astype(jnp.float32)
    scale = jnp.exp2(numbers[:, count:count + 1] - 14.0)
    return numbers[:, :count] * scale


def ring_order(count):
    return sorted(range(1, count), key=lambda d: -min(d, count - d))


def remote(src, dst, send_sem, recv_sem, device):
    return pltpu.make_async_remote_copy(
        src_ref=src, dst_ref=dst, send_sem=send_sem, recv_sem=recv_sem,
        device_id=device, device_id_type=MESH,
    )


def dot_nt(a, b):
    return lax.dot_general(a, b, NT, preferred_element_type=jnp.float32)


def kernel(
    rows, cols, blocks, factor_hbm, inverse_hbm, rhs_hbm, order_hbm, live_hbm, out,
    factor, inverse, cand, theirs, pieces, mine, panels, quarters, quarter, sixteenths, joined,
    b_own, b_pair, b_chip, b0_in, b0_all, b_line, b_turn, b_cross,
    part_out, part_in, stored, acc, tail_out, tail_in, rhs, order, live,
    factor_sem, inverse_sem, small_sem, pair_sems, b_sems, piece_sems, panel_sems, line_sems,
    b0_sems, b1_sems, part_sems, stored_sems, tail_sems,
):
    sections = len(factor)
    rows_dev, tile, width = factor[0].shape
    rhs_count = rhs.shape[0]
    chips = cols // 2
    piece = tile // chips
    r, c = lax.axis_index("row"), lax.axis_index("col")
    chip, core = lax.div(c, 2), lax.rem(c, 2)
    index = {tu: i for i, tu in enumerate(blocks)}

    small = (
        pltpu.make_async_copy(rhs_hbm, rhs, small_sem.at[0]),
        pltpu.make_async_copy(order_hbm, order, small_sem.at[1]),
        pltpu.make_async_copy(live_hbm, live, small_sem.at[2]),
    )
    for copy in small:
        copy.start()
    factor_loads = []
    for u in range(sections):
        copy = pltpu.make_async_copy(factor_hbm.at[u], factor[u], factor_sem.at[u])
        copy.start()
        factor_loads.append(copy)
    inverse_load = pltpu.make_async_copy(inverse_hbm, inverse, inverse_sem.at[0])
    inverse_load.start()

    barrier = pltpu.get_barrier_semaphore()
    for axis, me, count in (("row", r, rows), ("col", c, cols)):
        for d in range(1, count):
            pl.semaphore_signal(
                barrier, inc=1, device_id={axis: lax.rem(me + d, count)}, device_id_type=MESH
            )

    for copy in small:
        copy.wait()
    slots = [order[u] for u in range(sections)]
    locals_ = [lax.rem(s, rows_dev) for s in slots]
    root_core = [lax.rem(lax.div(s, rows_dev), 2) for s in slots]
    root_chip = [lax.div(s, 2 * rows_dev) for s in slots]
    row_ids = lax.broadcasted_iota(jnp.int32, (rhs_count, width), 0)
    limit = jnp.zeros((rhs_count, width), jnp.int32)
    for k in range(rhs_count):
        limit = jnp.where(row_ids == k, live[k], limit)

    for t in range(sections):
        picked = rhs[:, 0, :]
        for j in range(1, rows_dev):
            picked = jnp.where(locals_[t] == j, rhs[:, j, :], picked)
        b_own[t] = picked
    for copy in factor_loads + [inverse_load]:
        copy.wait()

    peers = [lax.rem(r + d, rows) for d in ring_order(rows)]
    others = [lax.rem(chip + d, chips) for d in range(1, chips)]

    def trail(t, sent):
        for j in range(rows_dev):
            update = dot_nt(sent, factor[t][j])
            if t == 0:
                acc[j] = update
            else:
                acc[j] += update

    @pl.when(core == 0)
    def _():
        pl.semaphore_wait(barrier, rows - 1 + cols - 1)
        pair = remote(b_own, b_pair, b_sems.at[0], b_sems.at[1], {"col": c + 1})
        pair.start()

        def merge(i):
            t, u = blocks[i]
            remote(
                theirs[i], theirs[i], pair_sems.at[0, i], pair_sems.at[1, i], {"col": c + 1}
            ).wait_recv()
            for s in range(0, tile, 256):
                own = factor[u][locals_[t], pl.ds(s, 256), :]
                cand[i][s:s + 256] = jnp.where(
                    root_core[t] == 1, theirs[i][s:s + 256], own
                )

        def span(index, size):
            return pl.ds(pl.multiple_of(index * size, size), size)

        def scatter(i):
            merge(i)
            for p in others:
                remote(
                    cand[i].at[span(p, piece)], pieces[i].at[chip],
                    piece_sems.at[0, i], piece_sems.at[1, i], {"col": 2 * p},
                ).start()
            pieces[i][chip] = cand[i][span(chip, piece)]

        def gather(i):
            t, u = blocks[i]
            some = pieces[i].at[pl.ds(0, chips - 1)]
            remote(some, some, piece_sems.at[0, i], piece_sems.at[1, i], {"col": c + 1}).wait_recv()
            mine[i] = pieces[i][root_chip[t]]
            for p in [chip] + others:
                remote(
                    mine.at[i], panels[i].at[span(chip, piece)],
                    panel_sems.at[0, i], panel_sems.at[1, i], {"col": 2 * p + 1},
                ).start()

        part = tile // SIDE
        ahead = [d for d in ring_order(SIDE)]

        def place(i):
            t, u = blocks[i]
            here = (lax.rem(chip, SIDE), lax.div(chip, SIDE))
            root = (lax.rem(root_chip[t], SIDE), lax.div(root_chip[t], SIDE))
            if i % 2:
                here, root = here[::-1], root[::-1]
                return here, root, lambda a, b: 2 * (a * SIDE + b)
            return here, root, lambda a, b: 2 * (b * SIDE + a)

        def line(i, stage, some):
            return remote(
                some, some, line_sems.at[stage, 0, i], line_sems.at[stage, 1, i], {"col": c + 1}
            )

        def first_line(i):
            merge(i)
            (a, b), root, core_of = place(i)
            for d in ahead:
                to = lax.rem(a + d, SIDE)
                remote(
                    cand[i].at[span(to, part)], quarters[i].at[a],
                    line_sems.at[0, 0, i], line_sems.at[0, 1, i], {"col": core_of(to, b)},
                ).start()
            quarters[i][a] = cand[i][span(a, part)]

        def second_line(i):
            (a, b), root, core_of = place(i)
            line(i, 0, quarters[i].at[pl.ds(0, SIDE - 1)]).wait_recv()
            quarter[i][...] = quarters[i][root[0]]
            for d in ahead:
                to = lax.rem(b + d, SIDE)
                remote(
                    quarter[i].at[span(to, piece)], sixteenths[i].at[b],
                    line_sems.at[1, 0, i], line_sems.at[1, 1, i], {"col": core_of(a, to)},
                ).start()
            sixteenths[i][b] = quarter[i][span(b, piece)]

        def third_line(i):
            (a, b), root, core_of = place(i)
            line(i, 1, sixteenths[i].at[pl.ds(0, SIDE - 1)]).wait_recv()
            joined[i][span(b, piece)] = sixteenths[i][root[1]]
            for d in ahead:
                remote(
                    joined[i].at[span(b, piece)], joined[i].at[span(b, piece)],
                    line_sems.at[2, 0, i], line_sems.at[2, 1, i],
                    {"col": core_of(a, lax.rem(b + d, SIDE))},
                ).start()

        def fourth_line(i):
            (a, b), root, core_of = place(i)
            line(i, 2, joined[i].at[pl.ds(0, part - piece)]).wait_recv()
            for d in ahead + [0]:
                remote(
                    joined[i], panels[i].at[span(a, part)],
                    panel_sems.at[0, i], panel_sems.at[1, i],
                    {"col": core_of(lax.rem(a + d, SIDE), b) + 1},
                ).start()

        direct = range(DIRECT)
        run = dict(
            s=scatter, g=gather, a=first_line, b=second_line, c=third_line, d=fourth_line
        )
        for op in ORDER.split():
            run[op[0]](int(op[1:]))

        for t in range(sections):
            remote(
                stored.at[t], stored.at[t], stored_sems.at[0, t], stored_sems.at[1, t],
                {"col": c + 1},
            ).wait_recv()
            trail(t, jnp.where(limit > t, stored[t], 0.0).astype(jnp.bfloat16))

        pair.wait_send()
        for i in range(len(blocks)):
            if i in direct:
                some = pieces[i].at[pl.ds(0, chips - 1)]
                remote(
                    some, some, piece_sems.at[0, i], piece_sems.at[1, i], {"col": c + 1}
                ).wait_send()
            else:
                line(i, 0, quarters[i].at[pl.ds(0, SIDE - 1)]).wait_send()
                line(i, 1, sixteenths[i].at[pl.ds(0, SIDE - 1)]).wait_send()
                line(i, 2, joined[i].at[pl.ds(0, part - piece)]).wait_send()
            remote(
                panels[i], panels[i], panel_sems.at[0, i], panel_sems.at[1, i], {"col": c + 1}
            ).wait_send()

    @pl.when(core == 1)
    def _():
        for i, (t, u) in enumerate(blocks):
            for s in range(0, tile, 256):
                cand[i][s:s + 256] = factor[u][locals_[t], pl.ds(s, 256), :]
        pl.semaphore_wait(barrier, rows - 1 + cols - 1)
        remote(b_own, b_pair, b_sems.at[0], b_sems.at[1], {"col": c - 1}).wait_recv()
        for t in range(sections):
            b_chip[t] = jnp.where(root_core[t] == 1, b_own[t], b_pair[t])
        for p in others:
            remote(
                b_chip.at[0], b0_in.at[chip], b0_sems.at[0, 0], b0_sems.at[1, 0],
                {"col": 2 * p + 1},
            ).start()
        chip_y, chip_x = lax.div(chip, SIDE), lax.rem(chip, SIDE)
        for d in ring_order(SIDE):
            to = chip_y * SIDE + lax.rem(chip_x + d, SIDE)
            remote(
                b_chip.at[pl.ds(1, sections - 1)], b_line.at[chip_x],
                b1_sems.at[0, 0], b1_sems.at[1, 0], {"col": 2 * to + 1},
            ).start()
        pairs = []
        for i in range(len(blocks)):
            copy = remote(
                cand[i], theirs[i], pair_sems.at[0, i], pair_sems.at[1, i], {"col": c - 1}
            )
            copy.start()
            pairs.append(copy)
        b0_in[chip] = b_chip[0]
        b_line[chip_x] = b_chip[1:]

        some = b0_in.at[pl.ds(0, chips - 1)]
        b0_wait = remote(some, some, b0_sems.at[0, 0], b0_sems.at[1, 0], {"col": c - 1})
        b0_wait.wait_recv()
        b0_all[r] = b0_in[root_chip[0]]
        for peer in peers:
            remote(
                b0_all.at[r], b0_all.at[r], b0_sems.at[0, 1], b0_sems.at[1, 1], {"row": peer}
            ).start()
        some = b_line.at[pl.ds(0, SIDE - 1)]
        line_wait = remote(some, some, b1_sems.at[0, 0], b1_sems.at[1, 0], {"col": c - 1})
        line_wait.wait_recv()
        for t in range(1, sections):
            b_turn[t - 1] = b_line[lax.rem(root_chip[t], SIDE), t - 1]
        for d in ring_order(SIDE):
            to = lax.rem(chip_y + d, SIDE) * SIDE + chip_x
            remote(
                b_turn, b_cross.at[chip_y], b1_sems.at[0, 1], b1_sems.at[1, 1],
                {"col": 2 * to + 1},
            ).start()
        b_cross[chip_y] = b_turn[...]
        some = b_cross.at[pl.ds(0, SIDE - 1)]
        cross_wait = remote(some, some, b1_sems.at[0, 1], b1_sems.at[1, 1], {"col": c - 1})

        def placed(t):
            value = b_cross[lax.div(root_chip[t], SIDE), t - 1]
            return jnp.concatenate([jnp.where(r == s, value, 0.0) for s in range(rows)], axis=1)

        some = b0_all.at[pl.ds(0, rows - 1)]
        b0_row = remote(some, some, b0_sems.at[0, 1], b0_sems.at[1, 1], {"col": c - 1})

        def panel(t, u):
            i = index[t, u]
            remote(
                panels[i], panels[i], panel_sems.at[0, i], panel_sems.at[1, i], {"col": c - 1}
            ).wait_recv()
            return panels[i][...]

        sents, pending = [], []
        own, older = None, None
        for t in range(sections):
            if t == 0:
                b0_row.wait_recv()
                remaining = jnp.concatenate([b0_all[s] for s in range(rows)], axis=1)
            else:
                remaining = -own
                for peer in reversed(peers):
                    remote(
                        part_out.at[t], part_in.at[t, peer], part_sems.at[0, t, peer],
                        part_sems.at[1, t, peer], {"row": peer},
                    ).wait_recv()
                    remaining = remaining - decode(part_in[t, peer], tile)
            kept = remaining[:, :width]
            for s in range(1, rows):
                kept = jnp.where(r == s, remaining[:, s * width:(s + 1) * width], kept)
            high = remaining.astype(jnp.bfloat16)
            rest = remaining - high.astype(jnp.float32)
            middle = rest.astype(jnp.bfloat16)
            low = (rest - middle.astype(jnp.float32)).astype(jnp.bfloat16)
            parts = dot_nt(jnp.concatenate([high, middle, low], axis=0), inverse[t])
            solved = (
                parts[2 * rhs_count:] + parts[rhs_count:2 * rhs_count]
            ) + parts[:rhs_count]
            is_live = limit > t
            sent = jnp.where(is_live, solved, 0.0).astype(jnp.bfloat16)
            sents.append(sent)
            if t + 1 < sections:
                if t == 0:
                    cross_wait.wait_recv()
                    older = -placed(1)
                own = dot_nt(sent, panel(t + 1, t)) + older
                part_out[t + 1] = encode(own, SPARE)
                for peer in peers:
                    copy = remote(
                        part_out.at[t + 1], part_in.at[t + 1, r], part_sems.at[0, t + 1, peer],
                        part_sems.at[1, t + 1, r], {"row": peer},
                    )
                    copy.start()
                    pending.append(copy)
            stored[t] = jnp.where(is_live, solved, kept)
            copy = remote(
                stored.at[t], stored.at[t], stored_sems.at[0, t], stored_sems.at[1, t],
                {"col": c - 1},
            )
            copy.start()
            pending.append(copy)
            trail(t, sent)
            if t + 2 < sections:
                older = -placed(t + 2)
                for u in range(t + 1):
                    older = older + dot_nt(sents[u], panel(t + 2, u))

        for wait in (b0_wait, b0_row, line_wait, cross_wait):
            wait.wait_send()
        for copy in pairs + pending:
            copy.wait_send()

    spans = []
    totals = [acc[j] for j in range(rows_dev)]
    for s in range(rows):
        spans.append([x[:, s * width:(s + 1) * width] for x in totals])
        tail_out[s] = jnp.concatenate(spans[s], axis=1).astype(jnp.bfloat16)
    tails = []
    for peer in peers:
        copy = remote(
            tail_out.at[peer], tail_in.at[r], tail_sems.at[0, peer], tail_sems.at[1, r],
            {"row": peer},
        )
        copy.start()
        tails.append(copy)
    values = []
    for j in range(rows_dev):
        total = spans[0][j]
        for s in range(1, rows):
            total = jnp.where(r == s, spans[s][j], total)
        values.append(rhs[:, j, :] - total)
    for peer in reversed(peers):
        remote(
            tail_out.at[peer], tail_in.at[peer], tail_sems.at[0, peer], tail_sems.at[1, peer],
            {"row": peer},
        ).wait_recv()
        other = tail_in[peer].astype(jnp.float32)
        for j in range(rows_dev):
            values[j] = values[j] - other[:, j * width:(j + 1) * width]
    for j in range(rows_dev):
        value = values[j]
        for t in range(sections):
            value = jnp.where(slots[t] == c * rows_dev + j, stored[t], value)
        out[:, j, :] = value
    for copy in tails:
        copy.wait_send()


def per_device(rows, cols, factor, diag_inverse, right_side, tile_order, live_segments):
    sections, width, tile = diag_inverse.shape
    rhs_count, rows_dev, _ = right_side.shape
    panel = jnp.transpose(factor, (1, 0, 2)).reshape(sections, rows_dev, tile, width)
    blocks = [(t, u) for t in range(1, sections) for u in range(t)]
    count, chips = len(blocks), cols // 2
    vmem = pl.BlockSpec(memory_space=pltpu.VMEM)
    hbm = pl.BlockSpec(memory_space=pl.ANY)
    f32, bf16, i16 = jnp.float32, jnp.bfloat16, jnp.int16
    dma = pltpu.SemaphoreType.DMA
    return pl.pallas_call(
        functools.partial(kernel, rows, cols, blocks),
        out_shape=jax.ShapeDtypeStruct(right_side.shape, f32),
        in_specs=[hbm] * 5,
        out_specs=vmem,
        scratch_shapes=[
            [pltpu.VMEM((rows_dev, tile, width), bf16)] * sections,
            pltpu.VMEM((sections, width, tile), bf16),
            [pltpu.VMEM((tile, width), bf16)] * count,
            [pltpu.VMEM((tile, width), bf16)] * count,
            [pltpu.VMEM((chips, tile // chips, width), bf16)] * count,
            pltpu.VMEM((count, tile // chips, width), bf16),
            [pltpu.VMEM((tile, width), bf16)] * count,
            [pltpu.VMEM((SIDE, tile // SIDE, width), bf16)] * count,
            [pltpu.VMEM((tile // SIDE, width), bf16)] * count,
            [pltpu.VMEM((SIDE, tile // chips, width), bf16)] * count,
            [pltpu.VMEM((tile // SIDE, width), bf16)] * count,
            pltpu.VMEM((sections, rhs_count, width), f32),
            pltpu.VMEM((sections, rhs_count, width), f32),
            pltpu.VMEM((sections, rhs_count, width), f32),
            pltpu.VMEM((chips, rhs_count, width), f32),
            pltpu.VMEM((rows, rhs_count, width), f32),
            pltpu.VMEM((SIDE, sections - 1, rhs_count, width), f32),
            pltpu.VMEM((sections - 1, rhs_count, width), f32),
            pltpu.VMEM((SIDE, sections - 1, rhs_count, width), f32),
            pltpu.VMEM((sections, rhs_count, tile + SPARE), i16),
            pltpu.VMEM((sections, rows, rhs_count, tile + SPARE), i16),
            pltpu.VMEM((sections, rhs_count, width), f32),
            pltpu.VMEM((rows_dev, rhs_count, tile), f32),
            pltpu.VMEM((rows, rhs_count, rows_dev * width), bf16),
            pltpu.VMEM((rows, rhs_count, rows_dev * width), bf16),
            pltpu.VMEM(right_side.shape, f32),
            pltpu.SMEM(tile_order.shape, jnp.int32),
            pltpu.SMEM(live_segments.shape, jnp.int32),
            dma((sections,)),
            dma((1,)),
            dma((3,)),
            dma((2, count)),
            dma((2,)),
            dma((2, count)),
            dma((2, count)),
            dma((3, 2, count)),
            dma((2, 2)),
            dma((2, 2)),
            dma((2, sections, rows)),
            dma((2, sections)),
            dma((2, rows)),
        ],
        compiler_params=pltpu.CompilerParams(
            collective_id=0, has_side_effects=True, vmem_limit_bytes=67043328
        ),
    )(panel, diag_inverse, right_side, tile_order, live_segments)


def solution(mesh):
    return jax.shard_map(
        functools.partial(per_device, mesh.shape["row"], mesh.shape["col"]),
        mesh=mesh,
        in_specs=(P("col", None, "row"), P(None, "row", None), P(None, "col", "row"), P(), P()),
        out_specs=P(None, "col", "row"),
        check_vma=False,
    )
```

```python
import functools
import jax
import jax.numpy as jnp
from jax import lax
from jax.experimental import pallas as pl
from jax.experimental.pallas import tpu as pltpu
from jax.sharding import PartitionSpec as P

MESH = pl.DeviceIdType.MESH
SPARE = 128
SIDE = 4
DEPTH = 4
NT = (((1,), (1,)), ((), ()))


def encode(value, spare):
    peak = jnp.max(jnp.abs(value), axis=1, keepdims=True)
    power = jnp.ceil(jnp.log2(jnp.maximum(peak, 1e-30)))
    coded = jnp.floor(value * jnp.exp2(14.0 - power) + 0.5)
    powers = jnp.broadcast_to(power, (value.shape[0], spare))
    both = jnp.concatenate([coded, powers], axis=1)
    return both.astype(jnp.int32).astype(jnp.int16)


def decode(coded, count):
    numbers = coded.astype(jnp.int32).astype(jnp.float32)
    scale = jnp.exp2(numbers[:, count:count + 1] - 14.0)
    return numbers[:, :count] * scale


def ring_order(count):
    return sorted(range(1, count), key=lambda d: -min(d, count - d))


def remote(src, dst, send_sem, recv_sem, device):
    return pltpu.make_async_remote_copy(
        src_ref=src, dst_ref=dst, send_sem=send_sem, recv_sem=recv_sem,
        device_id=device, device_id_type=MESH,
    )


def dot_nt(a, b):
    return lax.dot_general(a, b, NT, preferred_element_type=jnp.float32)


def kernel(
    rows, cols, blocks, factor_hbm, inverse_hbm, rhs_hbm, order_hbm, live_hbm, out,
    factor, inverse, cand, theirs, pieces, mine, panels,
    b_own, b_pair, b_chip, b0_in, b0_all, b_line, b_turn, b_cross,
    part_out, part_in, stored, acc, tail_out, tail_in, rhs, order, live,
    factor_sem, inverse_sem, small_sem, pair_sems, b_sems, piece_sems, panel_sems,
    b0_sems, b1_sems, part_sems, stored_sems, tail_sems,
):
    sections = len(factor)
    rows_dev, tile, width = factor[0].shape
    rhs_count = rhs.shape[0]
    chips = cols // 2
    piece = tile // chips
    r, c = lax.axis_index("row"), lax.axis_index("col")
    chip, core = lax.div(c, 2), lax.rem(c, 2)
    index = {tu: i for i, tu in enumerate(blocks)}

    small = (
        pltpu.make_async_copy(rhs_hbm, rhs, small_sem.at[0]),
        pltpu.make_async_copy(order_hbm, order, small_sem.at[1]),
        pltpu.make_async_copy(live_hbm, live, small_sem.at[2]),
    )
    for copy in small:
        copy.start()
    factor_loads = []
    for u in range(sections):
        copy = pltpu.make_async_copy(factor_hbm.at[u], factor[u], factor_sem.at[u])
        copy.start()
        factor_loads.append(copy)
    inverse_load = pltpu.make_async_copy(inverse_hbm, inverse, inverse_sem.at[0])
    inverse_load.start()

    barrier = pltpu.get_barrier_semaphore()
    for axis, me, count in (("row", r, rows), ("col", c, cols)):
        for d in range(1, count):
            pl.semaphore_signal(
                barrier, inc=1, device_id={axis: lax.rem(me + d, count)}, device_id_type=MESH
            )

    for copy in small:
        copy.wait()
    slots = [order[u] for u in range(sections)]
    locals_ = [lax.rem(s, rows_dev) for s in slots]
    root_core = [lax.rem(lax.div(s, rows_dev), 2) for s in slots]
    root_chip = [lax.div(s, 2 * rows_dev) for s in slots]
    row_ids = lax.broadcasted_iota(jnp.int32, (rhs_count, width), 0)
    limit = jnp.zeros((rhs_count, width), jnp.int32)
    for k in range(rhs_count):
        limit = jnp.where(row_ids == k, live[k], limit)

    for t in range(sections):
        picked = rhs[:, 0, :]
        for j in range(1, rows_dev):
            picked = jnp.where(locals_[t] == j, rhs[:, j, :], picked)
        b_own[t] = picked
    for copy in factor_loads + [inverse_load]:
        copy.wait()

    peers = [lax.rem(r + d, rows) for d in ring_order(rows)]
    others = [lax.rem(chip + d, chips) for d in range(1, chips)]

    def trail(t, sent):
        for j in range(rows_dev):
            update = dot_nt(sent, factor[t][j])
            if t == 0:
                acc[j] = update
            else:
                acc[j] += update

    @pl.when(core == 0)
    def _():
        pl.semaphore_wait(barrier, rows - 1 + cols - 1)
        pair = remote(b_own, b_pair, b_sems.at[0], b_sems.at[1], {"col": c + 1})
        pair.start()

        def merge(i):
            t, u = blocks[i]
            remote(
                theirs[i], theirs[i], pair_sems.at[0, i], pair_sems.at[1, i], {"col": c + 1}
            ).wait_recv()
            for s in range(0, tile, 256):
                own = factor[u][locals_[t], pl.ds(s, 256), :]
                cand[i][s:s + 256] = jnp.where(
                    root_core[t] == 1, theirs[i][s:s + 256], own
                )

        def span(index, size):
            return pl.ds(pl.multiple_of(index * size, size), size)

        def scatter(i):
            merge(i)
            for p in others:
                remote(
                    cand[i].at[span(p, piece)], pieces[i].at[chip],
                    piece_sems.at[0, i], piece_sems.at[1, i], {"col": 2 * p},
                ).start()
            pieces[i][chip] = cand[i][span(chip, piece)]

        def gather(i):
            t, u = blocks[i]
            some = pieces[i].at[pl.ds(0, chips - 1)]
            remote(some, some, piece_sems.at[0, i], piece_sems.at[1, i], {"col": c + 1}).wait_recv()
            mine[i] = pieces[i][root_chip[t]]
            for p in [chip] + others:
                remote(
                    mine.at[i], panels[i].at[span(chip, piece)],
                    panel_sems.at[0, i], panel_sems.at[1, i], {"col": 2 * p + 1},
                ).start()

        for i in range(DEPTH):
            scatter(i)
        for i in range(len(blocks)):
            gather(i)
            if i + DEPTH < len(blocks):
                scatter(i + DEPTH)

        for t in range(sections):
            remote(
                stored.at[t], stored.at[t], stored_sems.at[0, t], stored_sems.at[1, t],
                {"col": c + 1},
            ).wait_recv()
            trail(t, jnp.where(limit > t, stored[t], 0.0).astype(jnp.bfloat16))

        pair.wait_send()
        for i in range(len(blocks)):
            some = pieces[i].at[pl.ds(0, chips - 1)]
            remote(some, some, piece_sems.at[0, i], piece_sems.at[1, i], {"col": c + 1}).wait_send()
            remote(
                panels[i], panels[i], panel_sems.at[0, i], panel_sems.at[1, i], {"col": c + 1}
            ).wait_send()

    @pl.when(core == 1)
    def _():
        for i, (t, u) in enumerate(blocks):
            for s in range(0, tile, 256):
                cand[i][s:s + 256] = factor[u][locals_[t], pl.ds(s, 256), :]
        pl.semaphore_wait(barrier, rows - 1 + cols - 1)
        pairs = []
        for i in range(len(blocks)):
            copy = remote(
                cand[i], theirs[i], pair_sems.at[0, i], pair_sems.at[1, i], {"col": c - 1}
            )
            copy.start()
            pairs.append(copy)
        remote(b_own, b_pair, b_sems.at[0], b_sems.at[1], {"col": c - 1}).wait_recv()
        for t in range(sections):
            b_chip[t] = jnp.where(root_core[t] == 1, b_own[t], b_pair[t])
        for p in others:
            remote(
                b_chip.at[0], b0_in.at[chip], b0_sems.at[0, 0], b0_sems.at[1, 0],
                {"col": 2 * p + 1},
            ).start()
        chip_y, chip_x = lax.div(chip, SIDE), lax.rem(chip, SIDE)
        for d in ring_order(SIDE):
            to = chip_y * SIDE + lax.rem(chip_x + d, SIDE)
            remote(
                b_chip.at[pl.ds(1, sections - 1)], b_line.at[chip_x],
                b1_sems.at[0, 0], b1_sems.at[1, 0], {"col": 2 * to + 1},
            ).start()
        b0_in[chip] = b_chip[0]
        b_line[chip_x] = b_chip[1:]

        some = b0_in.at[pl.ds(0, chips - 1)]
        b0_wait = remote(some, some, b0_sems.at[0, 0], b0_sems.at[1, 0], {"col": c - 1})
        b0_wait.wait_recv()
        b0_all[r] = b0_in[root_chip[0]]
        for peer in peers:
            remote(
                b0_all.at[r], b0_all.at[r], b0_sems.at[0, 1], b0_sems.at[1, 1], {"row": peer}
            ).start()
        some = b_line.at[pl.ds(0, SIDE - 1)]
        line_wait = remote(some, some, b1_sems.at[0, 0], b1_sems.at[1, 0], {"col": c - 1})
        line_wait.wait_recv()
        for t in range(1, sections):
            b_turn[t - 1] = b_line[lax.rem(root_chip[t], SIDE), t - 1]
        for d in ring_order(SIDE):
            to = lax.rem(chip_y + d, SIDE) * SIDE + chip_x
            remote(
                b_turn, b_cross.at[chip_y], b1_sems.at[0, 1], b1_sems.at[1, 1],
                {"col": 2 * to + 1},
            ).start()
        b_cross[chip_y] = b_turn[...]
        some = b_cross.at[pl.ds(0, SIDE - 1)]
        cross_wait = remote(some, some, b1_sems.at[0, 1], b1_sems.at[1, 1], {"col": c - 1})

        def placed(t):
            value = b_cross[lax.div(root_chip[t], SIDE), t - 1]
            return jnp.concatenate([jnp.where(r == s, value, 0.0) for s in range(rows)], axis=1)

        some = b0_all.at[pl.ds(0, rows - 1)]
        b0_row = remote(some, some, b0_sems.at[0, 1], b0_sems.at[1, 1], {"col": c - 1})

        def panel(t, u):
            i = index[t, u]
            remote(
                panels[i], panels[i], panel_sems.at[0, i], panel_sems.at[1, i], {"col": c - 1}
            ).wait_recv()
            return panels[i][...]

        sents, pending = [], []
        own, older = None, None
        for t in range(sections):
            if t == 0:
                b0_row.wait_recv()
                remaining = jnp.concatenate([b0_all[s] for s in range(rows)], axis=1)
            else:
                remaining = -own
                for peer in reversed(peers):
                    remote(
                        part_out.at[t], part_in.at[t, peer], part_sems.at[0, t, peer],
                        part_sems.at[1, t, peer], {"row": peer},
                    ).wait_recv()
                    remaining = remaining - decode(part_in[t, peer], tile)
            kept = remaining[:, :width]
            for s in range(1, rows):
                kept = jnp.where(r == s, remaining[:, s * width:(s + 1) * width], kept)
            high = remaining.astype(jnp.bfloat16)
            rest = remaining - high.astype(jnp.float32)
            middle = rest.astype(jnp.bfloat16)
            low = (rest - middle.astype(jnp.float32)).astype(jnp.bfloat16)
            parts = dot_nt(jnp.concatenate([high, middle, low], axis=0), inverse[t])
            solved = (
                parts[2 * rhs_count:] + parts[rhs_count:2 * rhs_count]
            ) + parts[:rhs_count]
            is_live = limit > t
            sent = jnp.where(is_live, solved, 0.0).astype(jnp.bfloat16)
            sents.append(sent)
            if t + 1 < sections:
                if t == 0:
                    cross_wait.wait_recv()
                    older = -placed(1)
                own = dot_nt(sent, panel(t + 1, t)) + older
                part_out[t + 1] = encode(own, SPARE)
                for peer in peers:
                    copy = remote(
                        part_out.at[t + 1], part_in.at[t + 1, r], part_sems.at[0, t + 1, peer],
                        part_sems.at[1, t + 1, r], {"row": peer},
                    )
                    copy.start()
                    pending.append(copy)
            stored[t] = jnp.where(is_live, solved, kept)
            copy = remote(
                stored.at[t], stored.at[t], stored_sems.at[0, t], stored_sems.at[1, t],
                {"col": c - 1},
            )
            copy.start()
            pending.append(copy)
            trail(t, sent)
            if t + 2 < sections:
                older = -placed(t + 2)
                for u in range(t + 1):
                    older = older + dot_nt(sents[u], panel(t + 2, u))

        for wait in (b0_wait, b0_row, line_wait, cross_wait):
            wait.wait_send()
        for copy in pairs + pending:
            copy.wait_send()

    spans = []
    totals = [acc[j] for j in range(rows_dev)]
    for s in range(rows):
        spans.append([x[:, s * width:(s + 1) * width] for x in totals])
        tail_out[s] = jnp.concatenate(spans[s], axis=1).astype(jnp.bfloat16)
    tails = []
    for peer in peers:
        copy = remote(
            tail_out.at[peer], tail_in.at[r], tail_sems.at[0, peer], tail_sems.at[1, r],
            {"row": peer},
        )
        copy.start()
        tails.append(copy)
    values = []
    for j in range(rows_dev):
        total = spans[0][j]
        for s in range(1, rows):
            total = jnp.where(r == s, spans[s][j], total)
        values.append(rhs[:, j, :] - total)
    for peer in reversed(peers):
        remote(
            tail_out.at[peer], tail_in.at[peer], tail_sems.at[0, peer], tail_sems.at[1, peer],
            {"row": peer},
        ).wait_recv()
        other = tail_in[peer].astype(jnp.float32)
        for j in range(rows_dev):
            values[j] = values[j] - other[:, j * width:(j + 1) * width]
    for j in range(rows_dev):
        value = values[j]
        for t in range(sections):
            value = jnp.where(slots[t] == c * rows_dev + j, stored[t], value)
        out[:, j, :] = value
    for copy in tails:
        copy.wait_send()


def per_device(rows, cols, factor, diag_inverse, right_side, tile_order, live_segments):
    sections, width, tile = diag_inverse.shape
    rhs_count, rows_dev, _ = right_side.shape
    panel = jnp.transpose(factor, (1, 0, 2)).reshape(sections, rows_dev, tile, width)
    blocks = [(t, u) for t in range(1, sections) for u in range(t)]
    count, chips = len(blocks), cols // 2
    vmem = pl.BlockSpec(memory_space=pltpu.VMEM)
    hbm = pl.BlockSpec(memory_space=pl.ANY)
    f32, bf16, i16 = jnp.float32, jnp.bfloat16, jnp.int16
    dma = pltpu.SemaphoreType.DMA
    return pl.pallas_call(
        functools.partial(kernel, rows, cols, blocks),
        out_shape=jax.ShapeDtypeStruct(right_side.shape, f32),
        in_specs=[hbm] * 5,
        out_specs=vmem,
        scratch_shapes=[
            [pltpu.VMEM((rows_dev, tile, width), bf16)] * sections,
            pltpu.VMEM((sections, width, tile), bf16),
            [pltpu.VMEM((tile, width), bf16)] * count,
            [pltpu.VMEM((tile, width), bf16)] * count,
            [pltpu.VMEM((chips, tile // chips, width), bf16)] * count,
            pltpu.VMEM((count, tile // chips, width), bf16),
            [pltpu.VMEM((tile, width), bf16)] * count,
            pltpu.VMEM((sections, rhs_count, width), f32),
            pltpu.VMEM((sections, rhs_count, width), f32),
            pltpu.VMEM((sections, rhs_count, width), f32),
            pltpu.VMEM((chips, rhs_count, width), f32),
            pltpu.VMEM((rows, rhs_count, width), f32),
            pltpu.VMEM((SIDE, sections - 1, rhs_count, width), f32),
            pltpu.VMEM((sections - 1, rhs_count, width), f32),
            pltpu.VMEM((SIDE, sections - 1, rhs_count, width), f32),
            pltpu.VMEM((sections, rhs_count, tile + SPARE), i16),
            pltpu.VMEM((sections, rows, rhs_count, tile + SPARE), i16),
            pltpu.VMEM((sections, rhs_count, width), f32),
            pltpu.VMEM((rows_dev, rhs_count, tile), f32),
            pltpu.VMEM((rows, rhs_count, rows_dev * width), bf16),
            pltpu.VMEM((rows, rhs_count, rows_dev * width), bf16),
            pltpu.VMEM(right_side.shape, f32),
            pltpu.SMEM(tile_order.shape, jnp.int32),
            pltpu.SMEM(live_segments.shape, jnp.int32),
            dma((sections,)),
            dma((1,)),
            dma((3,)),
            dma((2, count)),
            dma((2,)),
            dma((2, count)),
            dma((2, count)),
            dma((2, 2)),
            dma((2, 2)),
            dma((2, sections, rows)),
            dma((2, sections)),
            dma((2, rows)),
        ],
        compiler_params=pltpu.CompilerParams(
            collective_id=0, has_side_effects=True, vmem_limit_bytes=67043328
        ),
    )(panel, diag_inverse, right_side, tile_order, live_segments)


def solution(mesh):
    return jax.shard_map(
        functools.partial(per_device, mesh.shape["row"], mesh.shape["col"]),
        mesh=mesh,
        in_specs=(P("col", None, "row"), P(None, "row", None), P(None, "col", "row"), P(), P()),
        out_specs=P(None, "col", "row"),
        check_vma=False,
    )
```

```python
import functools
import jax
import jax.numpy as jnp
from jax import lax
from jax.experimental import pallas as pl
from jax.experimental.pallas import tpu as pltpu
from jax.sharding import PartitionSpec as P

MESH = pl.DeviceIdType.MESH
SPARE = 128
SIDE = 4
DEPTH = 4
NT = (((1,), (1,)), ((), ()))


def encode(value, spare):
    peak = jnp.max(jnp.abs(value), axis=1, keepdims=True)
    power = jnp.ceil(jnp.log2(jnp.maximum(peak, 1e-30)))
    coded = jnp.floor(value * jnp.exp2(14.0 - power) + 0.5)
    powers = jnp.broadcast_to(power, (value.shape[0], spare))
    both = jnp.concatenate([coded, powers], axis=1)
    return both.astype(jnp.int32).astype(jnp.int16)


def decode(coded, count):
    numbers = coded.astype(jnp.int32).astype(jnp.float32)
    scale = jnp.exp2(numbers[:, count:count + 1] - 14.0)
    return numbers[:, :count] * scale


def ring_order(count):
    return sorted(range(1, count), key=lambda d: -min(d, count - d))


def remote(src, dst, send_sem, recv_sem, device):
    return pltpu.make_async_remote_copy(
        src_ref=src, dst_ref=dst, send_sem=send_sem, recv_sem=recv_sem,
        device_id=device, device_id_type=MESH,
    )


def dot_nt(a, b):
    return lax.dot_general(a, b, NT, preferred_element_type=jnp.float32)


def kernel(
    rows, cols, blocks, factor_hbm, inverse_hbm, rhs_hbm, order_hbm, live_hbm, out,
    factor, inverse, cand, theirs, pieces, mine, panels,
    b_own, b_pair, b_chip, b0_in, b0_all, b_line, b_turn, b_cross,
    part_out, part_in, stored, acc, tail_out, tail_in, mate_factor, mate_acc, mate_out, rhs, order, live,
    factor_sem, inverse_sem, small_sem, pair_sems, b_sems, piece_sems, panel_sems,
    b0_sems, b1_sems, part_sems, stored_sems, tail_sems, mate_sems, mate_tail_sems,
):
    sections = len(factor)
    rows_dev, tile, width = factor[0].shape
    rhs_count = rhs.shape[0]
    chips = cols // 2
    piece = tile // chips
    r, c = lax.axis_index("row"), lax.axis_index("col")
    chip, core = lax.div(c, 2), lax.rem(c, 2)
    index = {tu: i for i, tu in enumerate(blocks)}

    small = (
        pltpu.make_async_copy(rhs_hbm, rhs, small_sem.at[0]),
        pltpu.make_async_copy(order_hbm, order, small_sem.at[1]),
        pltpu.make_async_copy(live_hbm, live, small_sem.at[2]),
    )
    for copy in small:
        copy.start()
    factor_loads = []
    for u in range(sections):
        copy = pltpu.make_async_copy(factor_hbm.at[u], factor[u], factor_sem.at[u])
        copy.start()
        factor_loads.append(copy)
    inverse_load = pltpu.make_async_copy(inverse_hbm, inverse, inverse_sem.at[0])
    inverse_load.start()

    barrier = pltpu.get_barrier_semaphore()
    for axis, me, count in (("row", r, rows), ("col", c, cols)):
        for d in range(1, count):
            pl.semaphore_signal(
                barrier, inc=1, device_id={axis: lax.rem(me + d, count)}, device_id_type=MESH
            )

    for d in range(1, rows):
        pl.semaphore_signal(
            barrier, inc=1, device_id={"row": lax.rem(r + d, rows), "col": c + 1 - 2 * core},
            device_id_type=MESH,
        )

    for copy in small:
        copy.wait()
    slots = [order[u] for u in range(sections)]
    locals_ = [lax.rem(s, rows_dev) for s in slots]
    root_core = [lax.rem(lax.div(s, rows_dev), 2) for s in slots]
    root_chip = [lax.div(s, 2 * rows_dev) for s in slots]
    row_ids = lax.broadcasted_iota(jnp.int32, (rhs_count, width), 0)
    limit = jnp.zeros((rhs_count, width), jnp.int32)
    for k in range(rhs_count):
        limit = jnp.where(row_ids == k, live[k], limit)

    for t in range(sections):
        picked = rhs[:, 0, :]
        for j in range(1, rows_dev):
            picked = jnp.where(locals_[t] == j, rhs[:, j, :], picked)
        b_own[t] = picked
    for copy in factor_loads + [inverse_load]:
        copy.wait()

    peers = [lax.rem(r + d, rows) for d in ring_order(rows)]
    others = [lax.rem(chip + d, chips) for d in range(1, chips)]

    def trail(t, sent):
        for j in range(rows_dev):
            update = dot_nt(sent, factor[t][j])
            if t == 0:
                acc[j] = update
            else:
                acc[j] += update

    last = sections - 1

    def split(totals, to):
        for s in range(rows):
            spans = [x[:, s * width:(s + 1) * width] for x in totals]
            to[s] = jnp.concatenate(spans, axis=1).astype(jnp.bfloat16)

    def subtract(values, s):
        other = tail_in[s].astype(jnp.float32)
        return [x - other[:, j * width:(j + 1) * width] for j, x in enumerate(values)]

    def finish(values):
        for j in range(rows_dev):
            value = values[j]
            for t in range(sections):
                value = jnp.where(slots[t] == c * rows_dev + j, stored[t], value)
            out[:, j, :] = value

    @pl.when(core == 0)
    def _():
        pl.semaphore_wait(barrier, 2 * (rows - 1) + cols - 1)
        pair = remote(b_own, b_pair, b_sems.at[0], b_sems.at[1], {"col": c + 1})
        pair.start()
        mates = [
            remote(a, b, mate_sems.at[0, n], mate_sems.at[1, n], {"col": c + 1})
            for n, (a, b) in enumerate(((factor[last], mate_factor), (acc, mate_acc)))
        ]

        def merge(i):
            t, u = blocks[i]
            remote(
                theirs[i], theirs[i], pair_sems.at[0, i], pair_sems.at[1, i], {"col": c + 1}
            ).wait_recv()
            for s in range(0, tile, 256):
                own = factor[u][locals_[t], pl.ds(s, 256), :]
                cand[i][s:s + 256] = jnp.where(
                    root_core[t] == 1, theirs[i][s:s + 256], own
                )

        def span(index, size):
            return pl.ds(pl.multiple_of(index * size, size), size)

        def scatter(i):
            merge(i)
            for p in others:
                remote(
                    cand[i].at[span(p, piece)], pieces[i].at[chip],
                    piece_sems.at[0, i], piece_sems.at[1, i], {"col": 2 * p},
                ).start()
            pieces[i][chip] = cand[i][span(chip, piece)]

        def gather(i):
            t, u = blocks[i]
            some = pieces[i].at[pl.ds(0, chips - 1)]
            remote(some, some, piece_sems.at[0, i], piece_sems.at[1, i], {"col": c + 1}).wait_recv()
            mine[i] = pieces[i][root_chip[t]]
            for p in [chip] + others:
                remote(
                    mine.at[i], panels[i].at[span(chip, piece)],
                    panel_sems.at[0, i], panel_sems.at[1, i], {"col": 2 * p + 1},
                ).start()

        for i in range(DEPTH):
            scatter(i)
        for i in range(len(blocks)):
            gather(i)
            if i + DEPTH < len(blocks):
                scatter(i + DEPTH)

        for t in range(sections):
            remote(
                stored.at[t], stored.at[t], stored_sems.at[0, t], stored_sems.at[1, t],
                {"col": c + 1},
            ).wait_recv()
            if t == 1:
                mates[0].start()
            if t < last:
                trail(t, jnp.where(limit > t, stored[t], 0.0).astype(jnp.bfloat16))
            if t == last - 1:
                mates[1].start()

        values = [rhs[:, j, :] for j in range(rows_dev)]
        for s in [r] + peers[::-1]:
            remote(
                tail_in.at[s], tail_in.at[s], mate_tail_sems.at[s], tail_sems.at[1, s],
                {"col": c + 1},
            ).wait_recv()
            values = subtract(values, s)
        finish(values)
        for copy in mates:
            copy.wait_send()
        pair.wait_send()
        for i in range(len(blocks)):
            some = pieces[i].at[pl.ds(0, chips - 1)]
            remote(some, some, piece_sems.at[0, i], piece_sems.at[1, i], {"col": c + 1}).wait_send()
            remote(
                panels[i], panels[i], panel_sems.at[0, i], panel_sems.at[1, i], {"col": c + 1}
            ).wait_send()

    @pl.when(core == 1)
    def _():
        for i, (t, u) in enumerate(blocks):
            for s in range(0, tile, 256):
                cand[i][s:s + 256] = factor[u][locals_[t], pl.ds(s, 256), :]
        pl.semaphore_wait(barrier, 2 * (rows - 1) + cols - 1)
        pairs = []
        for i in range(len(blocks)):
            copy = remote(
                cand[i], theirs[i], pair_sems.at[0, i], pair_sems.at[1, i], {"col": c - 1}
            )
            copy.start()
            pairs.append(copy)
        remote(b_own, b_pair, b_sems.at[0], b_sems.at[1], {"col": c - 1}).wait_recv()
        for t in range(sections):
            b_chip[t] = jnp.where(root_core[t] == 1, b_own[t], b_pair[t])
        for p in others:
            remote(
                b_chip.at[0], b0_in.at[chip], b0_sems.at[0, 0], b0_sems.at[1, 0],
                {"col": 2 * p + 1},
            ).start()
        chip_y, chip_x = lax.div(chip, SIDE), lax.rem(chip, SIDE)
        for d in ring_order(SIDE):
            to = chip_y * SIDE + lax.rem(chip_x + d, SIDE)
            remote(
                b_chip.at[pl.ds(1, sections - 1)], b_line.at[chip_x],
                b1_sems.at[0, 0], b1_sems.at[1, 0], {"col": 2 * to + 1},
            ).start()
        b0_in[chip] = b_chip[0]
        b_line[chip_x] = b_chip[1:]

        some = b0_in.at[pl.ds(0, chips - 1)]
        b0_wait = remote(some, some, b0_sems.at[0, 0], b0_sems.at[1, 0], {"col": c - 1})
        b0_wait.wait_recv()
        b0_all[r] = b0_in[root_chip[0]]
        for peer in peers:
            remote(
                b0_all.at[r], b0_all.at[r], b0_sems.at[0, 1], b0_sems.at[1, 1], {"row": peer}
            ).start()
        some = b_line.at[pl.ds(0, SIDE - 1)]
        line_wait = remote(some, some, b1_sems.at[0, 0], b1_sems.at[1, 0], {"col": c - 1})
        line_wait.wait_recv()
        for t in range(1, sections):
            b_turn[t - 1] = b_line[lax.rem(root_chip[t], SIDE), t - 1]
        for d in ring_order(SIDE):
            to = lax.rem(chip_y + d, SIDE) * SIDE + chip_x
            remote(
                b_turn, b_cross.at[chip_y], b1_sems.at[0, 1], b1_sems.at[1, 1],
                {"col": 2 * to + 1},
            ).start()
        b_cross[chip_y] = b_turn[...]
        some = b_cross.at[pl.ds(0, SIDE - 1)]
        cross_wait = remote(some, some, b1_sems.at[0, 1], b1_sems.at[1, 1], {"col": c - 1})

        def placed(t):
            value = b_cross[lax.div(root_chip[t], SIDE), t - 1]
            return jnp.concatenate([jnp.where(r == s, value, 0.0) for s in range(rows)], axis=1)

        some = b0_all.at[pl.ds(0, rows - 1)]
        b0_row = remote(some, some, b0_sems.at[0, 1], b0_sems.at[1, 1], {"col": c - 1})

        def panel(t, u):
            i = index[t, u]
            remote(
                panels[i], panels[i], panel_sems.at[0, i], panel_sems.at[1, i], {"col": c - 1}
            ).wait_recv()
            return panels[i][...]

        mates = [
            remote(x, x, mate_sems.at[0, n], mate_sems.at[1, n], {"col": c - 1})
            for n, x in enumerate((mate_factor, mate_acc))
        ]
        sents, pending = [], []
        own, older = None, None
        for t in range(sections):
            if t == 0:
                b0_row.wait_recv()
                remaining = jnp.concatenate([b0_all[s] for s in range(rows)], axis=1)
            else:
                remaining = -own
                for peer in reversed(peers):
                    remote(
                        part_out.at[t], part_in.at[t, peer], part_sems.at[0, t, peer],
                        part_sems.at[1, t, peer], {"row": peer},
                    ).wait_recv()
                    remaining = remaining - decode(part_in[t, peer], tile)
            kept = remaining[:, :width]
            for s in range(1, rows):
                kept = jnp.where(r == s, remaining[:, s * width:(s + 1) * width], kept)
            high = remaining.astype(jnp.bfloat16)
            rest = remaining - high.astype(jnp.float32)
            middle = rest.astype(jnp.bfloat16)
            low = (rest - middle.astype(jnp.float32)).astype(jnp.bfloat16)
            parts = dot_nt(jnp.concatenate([high, middle, low], axis=0), inverse[t])
            solved = (
                parts[2 * rhs_count:] + parts[rhs_count:2 * rhs_count]
            ) + parts[:rhs_count]
            is_live = limit > t
            sent = jnp.where(is_live, solved, 0.0).astype(jnp.bfloat16)
            sents.append(sent)
            if t + 1 < sections:
                if t == 0:
                    cross_wait.wait_recv()
                    older = -placed(1)
                own = dot_nt(sent, panel(t + 1, t)) + older
                part_out[t + 1] = encode(own, SPARE)
                for peer in peers:
                    copy = remote(
                        part_out.at[t + 1], part_in.at[t + 1, r], part_sems.at[0, t + 1, peer],
                        part_sems.at[1, t + 1, r], {"row": peer},
                    )
                    copy.start()
                    pending.append(copy)
            if t == last:
                for copy in mates:
                    copy.wait_recv()
                totals = [acc[j] + dot_nt(sent, factor[t][j]) for j in range(rows_dev)]
                split(totals, tail_out)
                for peer in peers:
                    copy = remote(
                        tail_out.at[peer], tail_in.at[r], tail_sems.at[0, peer],
                        tail_sems.at[1, r], {"row": peer},
                    )
                    copy.start()
                    pending.append(copy)
                split(
                    [mate_acc[j] + dot_nt(sent, mate_factor[j]) for j in range(rows_dev)],
                    mate_out,
                )
                for peer in peers:
                    copy = remote(
                        mate_out.at[peer], tail_in.at[r], mate_tail_sems.at[peer],
                        tail_sems.at[1, r], {"row": peer, "col": c - 1},
                    )
                    copy.start()
                    pending.append(copy)
                copy = remote(
                    mate_out.at[r], tail_in.at[r], mate_tail_sems.at[r], tail_sems.at[1, r],
                    {"col": c - 1},
                )
                copy.start()
                pending.append(copy)
            stored[t] = jnp.where(is_live, solved, kept)
            copy = remote(
                stored.at[t], stored.at[t], stored_sems.at[0, t], stored_sems.at[1, t],
                {"col": c - 1},
            )
            copy.start()
            pending.append(copy)
            if t < last:
                trail(t, sent)
            if t + 2 < sections:
                older = -placed(t + 2)
                for u in range(t + 1):
                    older = older + dot_nt(sents[u], panel(t + 2, u))

        values = []
        for j in range(rows_dev):
            total = totals[j][:, :width]
            for s in range(1, rows):
                total = jnp.where(r == s, totals[j][:, s * width:(s + 1) * width], total)
            values.append(rhs[:, j, :] - total)
        for peer in reversed(peers):
            remote(
                tail_out.at[peer], tail_in.at[peer], tail_sems.at[0, peer],
                tail_sems.at[1, peer], {"row": peer},
            ).wait_recv()
            values = subtract(values, peer)
        finish(values)
        for wait in (b0_wait, b0_row, line_wait, cross_wait):
            wait.wait_send()
        for copy in pairs + pending:
            copy.wait_send()


def per_device(rows, cols, factor, diag_inverse, right_side, tile_order, live_segments):
    sections, width, tile = diag_inverse.shape
    rhs_count, rows_dev, _ = right_side.shape
    panel = jnp.transpose(factor, (1, 0, 2)).reshape(sections, rows_dev, tile, width)
    blocks = [(t, u) for t in range(1, sections) for u in range(t)]
    count, chips = len(blocks), cols // 2
    vmem = pl.BlockSpec(memory_space=pltpu.VMEM)
    hbm = pl.BlockSpec(memory_space=pl.ANY)
    f32, bf16, i16 = jnp.float32, jnp.bfloat16, jnp.int16
    dma = pltpu.SemaphoreType.DMA
    return pl.pallas_call(
        functools.partial(kernel, rows, cols, blocks),
        out_shape=jax.ShapeDtypeStruct(right_side.shape, f32),
        in_specs=[hbm] * 5,
        out_specs=vmem,
        scratch_shapes=[
            [pltpu.VMEM((rows_dev, tile, width), bf16)] * sections,
            pltpu.VMEM((sections, width, tile), bf16),
            [pltpu.VMEM((tile, width), bf16)] * count,
            [pltpu.VMEM((tile, width), bf16)] * count,
            [pltpu.VMEM((chips, tile // chips, width), bf16)] * count,
            pltpu.VMEM((count, tile // chips, width), bf16),
            [pltpu.VMEM((tile, width), bf16)] * count,
            pltpu.VMEM((sections, rhs_count, width), f32),
            pltpu.VMEM((sections, rhs_count, width), f32),
            pltpu.VMEM((sections, rhs_count, width), f32),
            pltpu.VMEM((chips, rhs_count, width), f32),
            pltpu.VMEM((rows, rhs_count, width), f32),
            pltpu.VMEM((SIDE, sections - 1, rhs_count, width), f32),
            pltpu.VMEM((sections - 1, rhs_count, width), f32),
            pltpu.VMEM((SIDE, sections - 1, rhs_count, width), f32),
            pltpu.VMEM((sections, rhs_count, tile + SPARE), i16),
            pltpu.VMEM((sections, rows, rhs_count, tile + SPARE), i16),
            pltpu.VMEM((sections, rhs_count, width), f32),
            pltpu.VMEM((rows_dev, rhs_count, tile), f32),
            pltpu.VMEM((rows, rhs_count, rows_dev * width), bf16),
            pltpu.VMEM((rows, rhs_count, rows_dev * width), bf16),
            pltpu.VMEM((rows_dev, tile, width), bf16),
            pltpu.VMEM((rows_dev, rhs_count, tile), f32),
            pltpu.VMEM((rows, rhs_count, rows_dev * width), bf16),
            pltpu.VMEM(right_side.shape, f32),
            pltpu.SMEM(tile_order.shape, jnp.int32),
            pltpu.SMEM(live_segments.shape, jnp.int32),
            dma((sections,)),
            dma((1,)),
            dma((3,)),
            dma((2, count)),
            dma((2,)),
            dma((2, count)),
            dma((2, count)),
            dma((2, 2)),
            dma((2, 2)),
            dma((2, sections, rows)),
            dma((2, sections)),
            dma((2, rows)),
            dma((2, 2)),
            dma((rows,)),
        ],
        compiler_params=pltpu.CompilerParams(
            collective_id=0, has_side_effects=True, vmem_limit_bytes=67043328
        ),
    )(panel, diag_inverse, right_side, tile_order, live_segments)


def solution(mesh):
    return jax.shard_map(
        functools.partial(per_device, mesh.shape["row"], mesh.shape["col"]),
        mesh=mesh,
        in_specs=(P("col", None, "row"), P(None, "row", None), P(None, "col", "row"), P(), P()),
        out_specs=P(None, "col", "row"),
        check_vma=False,
    )
```

```python
import functools
import jax
import jax.numpy as jnp
from jax import lax
from jax.experimental import pallas as pl
from jax.experimental.pallas import tpu as pltpu
from jax.sharding import PartitionSpec as P

MESH = pl.DeviceIdType.MESH
SPARE = 128
SIDE = 4
DEPTH = 4
NT = (((1,), (1,)), ((), ()))


def encode(value, spare):
    peak = jnp.max(jnp.abs(value), axis=1, keepdims=True)
    power = jnp.ceil(jnp.log2(jnp.maximum(peak, 1e-30)))
    coded = jnp.floor(value * jnp.exp2(14.0 - power) + 0.5)
    powers = jnp.broadcast_to(power, (value.shape[0], spare))
    both = jnp.concatenate([coded, powers], axis=1)
    return both.astype(jnp.int32).astype(jnp.int16)


def decode(coded, count):
    numbers = coded.astype(jnp.int32).astype(jnp.float32)
    scale = jnp.exp2(numbers[:, count:count + 1] - 14.0)
    return numbers[:, :count] * scale


def ring_order(count):
    return sorted(range(1, count), key=lambda d: -min(d, count - d))


def remote(src, dst, send_sem, recv_sem, device):
    return pltpu.make_async_remote_copy(
        src_ref=src, dst_ref=dst, send_sem=send_sem, recv_sem=recv_sem,
        device_id=device, device_id_type=MESH,
    )


def dot_nt(a, b):
    return lax.dot_general(a, b, NT, preferred_element_type=jnp.float32)


def kernel(
    rows, cols, blocks, factor_hbm, inverse_hbm, rhs_hbm, order_hbm, live_hbm, out,
    factor, inverse, cand, theirs, pieces, mine, panels,
    b_own, b_pair, b_chip, b0_in, b0_all, b_line, b_turn, b_cross,
    part_out, part_in, stored, acc, tail_out, tail_in, mate_factor, mate_acc, mate_out, rhs, order, live,
    factor_sem, inverse_sem, small_sem, pair_sems, b_sems, piece_sems, panel_sems,
    b0_sems, b1_sems, part_sems, stored_sems, tail_sems, mate_sems, mate_tail_sems,
):
    sections = len(factor)
    rows_dev, tile, width = factor[0].shape
    rhs_count = rhs.shape[0]
    chips = cols // 2
    piece = tile // chips
    r, c = lax.axis_index("row"), lax.axis_index("col")
    chip, core = lax.div(c, 2), lax.rem(c, 2)
    index = {tu: i for i, tu in enumerate(blocks)}

    barrier = pltpu.get_barrier_semaphore()
    for axis, me, count in (("row", r, rows), ("col", c, cols)):
        for d in range(1, count):
            pl.semaphore_signal(
                barrier, inc=1, device_id={axis: lax.rem(me + d, count)}, device_id_type=MESH
            )

    for d in range(1, rows):
        pl.semaphore_signal(
            barrier, inc=1, device_id={"row": lax.rem(r + d, rows), "col": c + 1 - 2 * core},
            device_id_type=MESH,
        )

    small = (
        pltpu.make_async_copy(rhs_hbm, rhs, small_sem.at[0]),
        pltpu.make_async_copy(order_hbm, order, small_sem.at[1]),
        pltpu.make_async_copy(live_hbm, live, small_sem.at[2]),
    )
    for copy in small:
        copy.start()
    factor_loads = []
    for u in range(sections):
        copy = pltpu.make_async_copy(factor_hbm.at[u], factor[u], factor_sem.at[u])
        copy.start()
        factor_loads.append(copy)
    inverse_load = pltpu.make_async_copy(inverse_hbm, inverse, inverse_sem.at[0])
    inverse_load.start()

    for copy in small:
        copy.wait()
    slots = [order[u] for u in range(sections)]
    locals_ = [lax.rem(s, rows_dev) for s in slots]
    root_core = [lax.rem(lax.div(s, rows_dev), 2) for s in slots]
    root_chip = [lax.div(s, 2 * rows_dev) for s in slots]
    row_ids = lax.broadcasted_iota(jnp.int32, (rhs_count, width), 0)
    limit = jnp.zeros((rhs_count, width), jnp.int32)
    for k in range(rhs_count):
        limit = jnp.where(row_ids == k, live[k], limit)

    for t in range(sections):
        picked = rhs[:, 0, :]
        for j in range(1, rows_dev):
            picked = jnp.where(locals_[t] == j, rhs[:, j, :], picked)
        b_own[t] = picked
    for copy in factor_loads + [inverse_load]:
        copy.wait()

    peers = [lax.rem(r + d, rows) for d in ring_order(rows)]
    others = [lax.rem(chip + d, chips) for d in range(1, chips)]

    def trail(t, sent):
        for j in range(rows_dev):
            update = dot_nt(sent, factor[t][j])
            if t == 0:
                acc[j] = update
            else:
                acc[j] += update

    last = sections - 1

    def split(totals, to):
        for s in range(rows):
            spans = [x[:, s * width:(s + 1) * width] for x in totals]
            to[s] = jnp.concatenate(spans, axis=1).astype(jnp.bfloat16)

    def subtract(values, s):
        other = tail_in[s].astype(jnp.float32)
        return [x - other[:, j * width:(j + 1) * width] for j, x in enumerate(values)]

    def finish(values):
        for j in range(rows_dev):
            value = values[j]
            for t in range(sections):
                value = jnp.where(slots[t] == c * rows_dev + j, stored[t], value)
            out[:, j, :] = value

    @pl.when(core == 0)
    def _():
        pl.semaphore_wait(barrier, 2 * (rows - 1) + cols - 1)
        pair = remote(b_own, b_pair, b_sems.at[0], b_sems.at[1], {"col": c + 1})
        pair.start()
        mates = [
            remote(a, b, mate_sems.at[0, n], mate_sems.at[1, n], {"col": c + 1})
            for n, (a, b) in enumerate(((factor[last], mate_factor), (acc, mate_acc)))
        ]

        def merge(i):
            t, u = blocks[i]
            remote(
                theirs[i], theirs[i], pair_sems.at[0, i], pair_sems.at[1, i], {"col": c + 1}
            ).wait_recv()
            for s in range(0, tile, 256):
                own = factor[u][locals_[t], pl.ds(s, 256), :]
                cand[i][s:s + 256] = jnp.where(
                    root_core[t] == 1, theirs[i][s:s + 256], own
                )

        def span(index, size):
            return pl.ds(pl.multiple_of(index * size, size), size)

        def scatter(i):
            merge(i)
            for p in others:
                remote(
                    cand[i].at[span(p, piece)], pieces[i].at[chip],
                    piece_sems.at[0, i], piece_sems.at[1, i], {"col": 2 * p},
                ).start()
            pieces[i][chip] = cand[i][span(chip, piece)]

        def gather(i):
            t, u = blocks[i]
            some = pieces[i].at[pl.ds(0, chips - 1)]
            remote(some, some, piece_sems.at[0, i], piece_sems.at[1, i], {"col": c + 1}).wait_recv()
            mine[i] = pieces[i][root_chip[t]]
            for p in [chip] + others:
                remote(
                    mine.at[i], panels[i].at[span(chip, piece)],
                    panel_sems.at[0, i], panel_sems.at[1, i], {"col": 2 * p + 1},
                ).start()

        for i in range(DEPTH):
            scatter(i)
        for i in range(len(blocks)):
            gather(i)
            if i + DEPTH < len(blocks):
                scatter(i + DEPTH)

        for t in range(sections):
            remote(
                stored.at[t], stored.at[t], stored_sems.at[0, t], stored_sems.at[1, t],
                {"col": c + 1},
            ).wait_recv()
            if t == 1:
                mates[0].start()
            if t < last:
                trail(t, jnp.where(limit > t, stored[t], 0.0).astype(jnp.bfloat16))
            if t == last - 1:
                mates[1].start()

        values = [rhs[:, j, :] for j in range(rows_dev)]
        for s in [r] + peers[::-1]:
            remote(
                tail_in.at[s], tail_in.at[s], mate_tail_sems.at[s], tail_sems.at[1, s],
                {"col": c + 1},
            ).wait_recv()
            values = subtract(values, s)
        finish(values)
        for copy in mates:
            copy.wait_send()
        pair.wait_send()
        for i in range(len(blocks)):
            some = pieces[i].at[pl.ds(0, chips - 1)]
            remote(some, some, piece_sems.at[0, i], piece_sems.at[1, i], {"col": c + 1}).wait_send()
            remote(
                panels[i], panels[i], panel_sems.at[0, i], panel_sems.at[1, i], {"col": c + 1}
            ).wait_send()

    @pl.when(core == 1)
    def _():
        for i, (t, u) in enumerate(blocks):
            for s in range(0, tile, 256):
                cand[i][s:s + 256] = factor[u][locals_[t], pl.ds(s, 256), :]
        pl.semaphore_wait(barrier, 2 * (rows - 1) + cols - 1)
        pairs = []
        for i in range(len(blocks)):
            copy = remote(
                cand[i], theirs[i], pair_sems.at[0, i], pair_sems.at[1, i], {"col": c - 1}
            )
            copy.start()
            pairs.append(copy)
        remote(b_own, b_pair, b_sems.at[0], b_sems.at[1], {"col": c - 1}).wait_recv()
        for t in range(sections):
            b_chip[t] = jnp.where(root_core[t] == 1, b_own[t], b_pair[t])
        for p in others:
            remote(
                b_chip.at[0], b0_in.at[chip], b0_sems.at[0, 0], b0_sems.at[1, 0],
                {"col": 2 * p + 1},
            ).start()
        chip_y, chip_x = lax.div(chip, SIDE), lax.rem(chip, SIDE)
        for d in ring_order(SIDE):
            to = chip_y * SIDE + lax.rem(chip_x + d, SIDE)
            remote(
                b_chip.at[pl.ds(1, sections - 1)], b_line.at[chip_x],
                b1_sems.at[0, 0], b1_sems.at[1, 0], {"col": 2 * to + 1},
            ).start()
        b0_in[chip] = b_chip[0]
        b_line[chip_x] = b_chip[1:]

        some = b0_in.at[pl.ds(0, chips - 1)]
        b0_wait = remote(some, some, b0_sems.at[0, 0], b0_sems.at[1, 0], {"col": c - 1})
        b0_wait.wait_recv()
        b0_all[r] = b0_in[root_chip[0]]
        for peer in peers:
            remote(
                b0_all.at[r], b0_all.at[r], b0_sems.at[0, 1], b0_sems.at[1, 1], {"row": peer}
            ).start()
        some = b_line.at[pl.ds(0, SIDE - 1)]
        line_wait = remote(some, some, b1_sems.at[0, 0], b1_sems.at[1, 0], {"col": c - 1})
        line_wait.wait_recv()
        for t in range(1, sections):
            b_turn[t - 1] = b_line[lax.rem(root_chip[t], SIDE), t - 1]
        for d in ring_order(SIDE):
            to = lax.rem(chip_y + d, SIDE) * SIDE + chip_x
            remote(
                b_turn, b_cross.at[chip_y], b1_sems.at[0, 1], b1_sems.at[1, 1],
                {"col": 2 * to + 1},
            ).start()
        b_cross[chip_y] = b_turn[...]
        some = b_cross.at[pl.ds(0, SIDE - 1)]
        cross_wait = remote(some, some, b1_sems.at[0, 1], b1_sems.at[1, 1], {"col": c - 1})

        def placed(t):
            value = b_cross[lax.div(root_chip[t], SIDE), t - 1]
            return jnp.concatenate([jnp.where(r == s, value, 0.0) for s in range(rows)], axis=1)

        some = b0_all.at[pl.ds(0, rows - 1)]
        b0_row = remote(some, some, b0_sems.at[0, 1], b0_sems.at[1, 1], {"col": c - 1})

        def panel(t, u):
            i = index[t, u]
            remote(
                panels[i], panels[i], panel_sems.at[0, i], panel_sems.at[1, i], {"col": c - 1}
            ).wait_recv()
            return panels[i][...]

        mates = [
            remote(x, x, mate_sems.at[0, n], mate_sems.at[1, n], {"col": c - 1})
            for n, x in enumerate((mate_factor, mate_acc))
        ]
        sents, pending = [], []
        own, older = None, None
        for t in range(sections):
            if t == 0:
                b0_row.wait_recv()
                remaining = jnp.concatenate([b0_all[s] for s in range(rows)], axis=1)
            else:
                remaining = -own
                for peer in reversed(peers):
                    remote(
                        part_out.at[t], part_in.at[t, peer], part_sems.at[0, t, peer],
                        part_sems.at[1, t, peer], {"row": peer},
                    ).wait_recv()
                    remaining = remaining - decode(part_in[t, peer], tile)
            kept = remaining[:, :width]
            for s in range(1, rows):
                kept = jnp.where(r == s, remaining[:, s * width:(s + 1) * width], kept)
            high = remaining.astype(jnp.bfloat16)
            rest = remaining - high.astype(jnp.float32)
            middle = rest.astype(jnp.bfloat16)
            low = (rest - middle.astype(jnp.float32)).astype(jnp.bfloat16)
            parts = dot_nt(jnp.concatenate([high, middle, low], axis=0), inverse[t])
            solved = (
                parts[2 * rhs_count:] + parts[rhs_count:2 * rhs_count]
            ) + parts[:rhs_count]
            is_live = limit > t
            sent = jnp.where(is_live, solved, 0.0).astype(jnp.bfloat16)
            sents.append(sent)
            if t + 1 < sections:
                if t == 0:
                    cross_wait.wait_recv()
                    older = -placed(1)
                own = dot_nt(sent, panel(t + 1, t)) + older
                part_out[t + 1] = encode(own, SPARE)
                for peer in peers:
                    copy = remote(
                        part_out.at[t + 1], part_in.at[t + 1, r], part_sems.at[0, t + 1, peer],
                        part_sems.at[1, t + 1, r], {"row": peer},
                    )
                    copy.start()
                    pending.append(copy)
            if t == last:
                for copy in mates:
                    copy.wait_recv()
                totals = [acc[j] + dot_nt(sent, factor[t][j]) for j in range(rows_dev)]
                split(totals, tail_out)
                for peer in peers:
                    copy = remote(
                        tail_out.at[peer], tail_in.at[r], tail_sems.at[0, peer],
                        tail_sems.at[1, r], {"row": peer},
                    )
                    copy.start()
                    pending.append(copy)
                split(
                    [mate_acc[j] + dot_nt(sent, mate_factor[j]) for j in range(rows_dev)],
                    mate_out,
                )
                for peer in peers:
                    copy = remote(
                        mate_out.at[peer], tail_in.at[r], mate_tail_sems.at[peer],
                        tail_sems.at[1, r], {"row": peer, "col": c - 1},
                    )
                    copy.start()
                    pending.append(copy)
                copy = remote(
                    mate_out.at[r], tail_in.at[r], mate_tail_sems.at[r], tail_sems.at[1, r],
                    {"col": c - 1},
                )
                copy.start()
                pending.append(copy)
            stored[t] = jnp.where(is_live, solved, kept)
            copy = remote(
                stored.at[t], stored.at[t], stored_sems.at[0, t], stored_sems.at[1, t],
                {"col": c - 1},
            )
            copy.start()
            pending.append(copy)
            if t < last:
                trail(t, sent)
            if t + 2 < sections:
                older = -placed(t + 2)
                for u in range(t + 1):
                    older = older + dot_nt(sents[u], panel(t + 2, u))

        values = []
        for j in range(rows_dev):
            total = totals[j][:, :width]
            for s in range(1, rows):
                total = jnp.where(r == s, totals[j][:, s * width:(s + 1) * width], total)
            values.append(rhs[:, j, :] - total)
        for peer in reversed(peers):
            remote(
                tail_out.at[peer], tail_in.at[peer], tail_sems.at[0, peer],
                tail_sems.at[1, peer], {"row": peer},
            ).wait_recv()
            values = subtract(values, peer)
        finish(values)
        for wait in (b0_wait, b0_row, line_wait, cross_wait):
            wait.wait_send()
        for copy in pairs + pending:
            copy.wait_send()


def per_device(rows, cols, factor, diag_inverse, right_side, tile_order, live_segments):
    sections, width, tile = diag_inverse.shape
    rhs_count, rows_dev, _ = right_side.shape
    panel = jnp.transpose(factor, (1, 0, 2)).reshape(sections, rows_dev, tile, width)
    blocks = [(t, u) for t in range(1, sections) for u in range(t)]
    count, chips = len(blocks), cols // 2
    vmem = pl.BlockSpec(memory_space=pltpu.VMEM)
    hbm = pl.BlockSpec(memory_space=pl.ANY)
    f32, bf16, i16 = jnp.float32, jnp.bfloat16, jnp.int16
    dma = pltpu.SemaphoreType.DMA
    return pl.pallas_call(
        functools.partial(kernel, rows, cols, blocks),
        out_shape=jax.ShapeDtypeStruct(right_side.shape, f32),
        in_specs=[hbm] * 5,
        out_specs=vmem,
        scratch_shapes=[
            [pltpu.VMEM((rows_dev, tile, width), bf16)] * sections,
            pltpu.VMEM((sections, width, tile), bf16),
            [pltpu.VMEM((tile, width), bf16)] * count,
            [pltpu.VMEM((tile, width), bf16)] * count,
            [pltpu.VMEM((chips, tile // chips, width), bf16)] * count,
            pltpu.VMEM((count, tile // chips, width), bf16),
            [pltpu.VMEM((tile, width), bf16)] * count,
            pltpu.VMEM((sections, rhs_count, width), f32),
            pltpu.VMEM((sections, rhs_count, width), f32),
            pltpu.VMEM((sections, rhs_count, width), f32),
            pltpu.VMEM((chips, rhs_count, width), f32),
            pltpu.VMEM((rows, rhs_count, width), f32),
            pltpu.VMEM((SIDE, sections - 1, rhs_count, width), f32),
            pltpu.VMEM((sections - 1, rhs_count, width), f32),
            pltpu.VMEM((SIDE, sections - 1, rhs_count, width), f32),
            pltpu.VMEM((sections, rhs_count, tile + SPARE), i16),
            pltpu.VMEM((sections, rows, rhs_count, tile + SPARE), i16),
            pltpu.VMEM((sections, rhs_count, width), f32),
            pltpu.VMEM((rows_dev, rhs_count, tile), f32),
            pltpu.VMEM((rows, rhs_count, rows_dev * width), bf16),
            pltpu.VMEM((rows, rhs_count, rows_dev * width), bf16),
            pltpu.VMEM((rows_dev, tile, width), bf16),
            pltpu.VMEM((rows_dev, rhs_count, tile), f32),
            pltpu.VMEM((rows, rhs_count, rows_dev * width), bf16),
            pltpu.VMEM(right_side.shape, f32),
            pltpu.SMEM(tile_order.shape, jnp.int32),
            pltpu.SMEM(live_segments.shape, jnp.int32),
            dma((sections,)),
            dma((1,)),
            dma((3,)),
            dma((2, count)),
            dma((2,)),
            dma((2, count)),
            dma((2, count)),
            dma((2, 2)),
            dma((2, 2)),
            dma((2, sections, rows)),
            dma((2, sections)),
            dma((2, rows)),
            dma((2, 2)),
            dma((rows,)),
        ],
        compiler_params=pltpu.CompilerParams(
            collective_id=0, has_side_effects=True, vmem_limit_bytes=67043328
        ),
    )(panel, diag_inverse, right_side, tile_order, live_segments)


def solution(mesh):
    return jax.shard_map(
        functools.partial(per_device, mesh.shape["row"], mesh.shape["col"]),
        mesh=mesh,
        in_specs=(P("col", None, "row"), P(None, "row", None), P(None, "col", "row"), P(), P()),
        out_specs=P(None, "col", "row"),
        check_vma=False,
    )
```
